32 devices in a mesh: tok: 16 (over z, y, x), exp: 2 (over core).
Axes of the slice: x: 2, y: 2, z: 4, core: 2. Of those that a mesh axis runs over, the one named last changes fastest.
Arguments:
- activations: bfloat16 [384, 14336], P(('tok', 'exp')), may hold values from -6 to 6
- expert_ids: int32 [384, 2], P(('tok', 'exp')), may hold values from 0 to 7, all different within a row; in each aligned block of 12 rows (0 to 11, 12 to 23, ...) at most 4 rows name the same one
Outputs:
- hessian: float32 [2, 14336, 14336], P('exp', 'tok')
The draws below stay inside these ranges and needn't reach their ends.
Inputs may be any that keep to these rules, and one draw needn't show every extreme that they name: `expert_ids`: each row names 2 different experts. Among the 12 rows of one device no expert is named more than 4 times, some expert exactly 4 times; every expert is named by some row.
All inputs are finite; a program needn't handle non-finite values.
Results may differ from the reference program's by a relative error of at most 0.0003.
Values may be sent and summed in bfloat16 or wider, within the bound.
No kernel may reach another device: no remote copies, remote signals or barrier semaphores. Data moves between devices by JAX's collectives and lax.ppermute only.
A program may use at most 128 MiB of HBM per device.

```python
import math
import jax
import jax.numpy as jnp
import numpy as np
from jax import lax

FF = 14336
NUM_EXPERTS = 8
TOP = 2
TOK_DEV = 12
CAP = 4
EXPERTS = 2
TOKENS = 384


def block_scale(stream_key, dims, shards, low, high):
    loudness, own = 1.0, jax.random.fold_in(stream_key, 6)
    for dim, shards_of in shards:
        steps = jnp.exp(jax.random.uniform(jax.random.fold_in(own, dim), (shards_of,), jnp.float32, low / len(shards), high / len(shards)))
        loudness = loudness * jnp.repeat(steps, dims[dim] // shards_of).reshape([-1 if axis == dim else 1 for axis in range(len(dims))])
    return loudness


def routed_block(key, own, number, rows, count, top, limit, slope):
    sequence = jax.random.permutation(key, count)
    heavy_load, common = shares(count, rows * top, limit, slope, True), shares(count, rows * top, limit, slope, False)
    places = jnp.arange(count)

    def named(lengths, rotation):
        used = int((lengths > 0).sum())
        fixed = max(1, used // 4)
        passed = fixed + (places - fixed + rotation * (used - fixed)) % max(1, count - fixed)
        return jnp.zeros((count,), jnp.int32).at[sequence[jnp.where(places < fixed, places, passed)]].set(jnp.asarray(lengths, jnp.int32))

    lengths = jnp.where(number % 4 == 0, named(heavy_load, number // 4), named(common, number - number // 4 - 1))
    mixed = jax.random.permutation(jax.random.fold_in(own, 3), count)
    donor, receiver = mixed[0:count // 2 * 2:2], mixed[1:count // 2 * 2:2]
    slack = jnp.minimum(lengths[donor] - 1, limit - lengths[receiver]) // 2
    slack = jnp.where((donor == sequence[0]) | (receiver == sequence[0]) | (lengths[receiver] == 0), 0, jnp.maximum(slack, 0))
    passed = jax.random.randint(jax.random.fold_in(own, 4), (count // 2,), 0, 1 << 20) % (slack + 1)
    lengths = lengths.at[donor].add(-passed).at[receiver].add(passed)
    labels = jnp.searchsorted(jnp.cumsum(lengths), jnp.arange(rows * top), side="right").astype(jnp.int32)
    table = labels.reshape(top, rows).T
    table = table[jax.random.permutation(jax.random.fold_in(own, 1), rows)]
    rotation = jax.random.randint(jax.random.fold_in(own, 2), (rows, 1), 0, top)
    return jnp.take_along_axis(table, (jnp.arange(top)[None, :] + rotation) % top, axis=1)


def shares(count, total, bound, lean, full):
    weights = [(1 << 20) // math.isqrt(grade ** lean) + 1 for grade in range(1, count + 1)]
    largest = bound if full else min(bound, max(-(-total // count), total * weights[0] // sum(weights)))
    least = 1 if total - largest >= count - 1 else 0
    given, rest = [largest] + [least] * (count - 1), total - largest - least * (count - 1)
    while rest > 0:
        movable = [i for i in range(1, count) if given[i] < largest] or [i for i in range(1, count) if given[i] < bound]
        pool, budget = sum([weights[i] for i in movable]), rest
        for i in movable:
            addition = min(bound - given[i], max(1, budget * weights[i] // pool), rest)
            given[i] = given[i] + addition
            rest = rest - addition
    return np.array(given)


def normal_values(rng, dims, spread, most, shards=(), held_as=jnp.bfloat16):
    drawn = spread * jax.random.normal(rng, dims, jnp.float32)
    if shards:
        drawn = drawn * block_scale(rng, dims, shards, -0.22, 0.18)
    return jnp.clip(drawn, -most, most).astype(held_as)


def setup_inputs(seed: int = 0) -> dict:
    splits = jax.random.split(jax.random.key(seed), 3)
    activations = normal_values(splits[0], (TOKENS, FF), 1.0, 6.0, ((0, 32),))
    expert_ids_keys = jax.random.split(jax.random.fold_in(splits[1], 1), TOKENS // TOK_DEV)
    expert_ids_turns = jax.random.permutation(jax.random.fold_in(splits[1], 3), TOKENS // TOK_DEV)
    expert_ids = jax.vmap(lambda own, number: routed_block(jax.random.fold_in(splits[1], 2), own, number, TOK_DEV, NUM_EXPERTS, TOP, CAP, 2))(expert_ids_keys, expert_ids_turns).reshape((TOKENS, TOP))
    return dict(activations=activations, expert_ids=expert_ids)


def reference(activations, expert_ids):
    features = activations.astype(jnp.float32)

    def one_expert(expert):
        routed = jnp.any(expert_ids == expert, axis=1).astype(jnp.float32)
        count = jnp.sum(routed)
        masked = features * routed[:, None]
        gram = jnp.dot(masked.T, features, precision=lax.Precision.HIGHEST, preferred_element_type=jnp.float32)
        return gram * (2.0 / count)

    return lax.map(one_expert, jnp.arange(EXPERTS, dtype=jnp.int32))
```

```python
import functools

import jax
import jax.numpy as jnp
from jax import lax
from jax.experimental import pallas as pl
from jax.experimental.pallas import tpu as pltpu
from jax.sharding import PartitionSpec as P

CAP = 4
LANES = 128
F32 = jnp.float32
BF16 = jnp.bfloat16


def tok_dims(mesh):
    n = mesh.shape["tok"]
    try:
        line = [tuple(d.coords) for d in mesh.devices.reshape(n, -1)[:, 0]]
        found = []
        for axis in range(3):
            size = len({c[axis] for c in line})
            if size > 1:
                stride = next(t for t in range(n) if line[t][axis] != line[0][axis])
                found.append((stride, size))
        sizes = [size for _, size in sorted(found, reverse=True)]
    except AttributeError:
        sizes = []
        while n > 1:
            part = 2 if n % 2 == 0 and len(sizes) < 2 else n
            sizes.append(part)
            n //= part
        sizes = sizes[::-1]
    while len(sizes) > 3:
        sizes = [sizes[0] * sizes[1]] + sizes[2:]
    return tuple(sizes + [1] * (3 - len(sizes)))


def slots_kernel(where, ids, act, out, *, experts, blocks, chunk):
    me, z = where[0], where[1]
    rows = act.shape[0]
    earlier = (
        lax.broadcasted_iota(jnp.int32, (rows, rows), 1) < lax.broadcasted_iota(jnp.int32, (rows, rows), 0)
    ).astype(F32)
    slot = lax.broadcasted_iota(jnp.int32, (rows, LANES), 1)
    for j in range(experts):
        expert = lax.rem(me + j, experts)
        hit = jnp.max((ids[...] == expert).astype(F32), axis=1, keepdims=True)
        wide = jnp.broadcast_to(hit, (rows, LANES))
        rank = jnp.dot(earlier, wide, preferred_element_type=F32)
        place = jnp.where((wide > 0.5) & (rank.astype(jnp.int32) == slot), 1.0, 0.0)
        place = place.T[:CAP].astype(BF16)
        for b in range(blocks):
            source = pl.multiple_of(comb(z, b, blocks) * chunk, LANES)
            out[j, :, b * chunk : (b + 1) * chunk] = jnp.dot(
                place, act[:, pl.ds(source, chunk)], preferred_element_type=F32
            ).astype(BF16)
        out[j, :, blocks * chunk :] = jnp.broadcast_to(
            jnp.sum(place.astype(F32), axis=1, keepdims=True), (CAP, LANES)
        ).astype(BF16)


def comb(a, b, n):
    return a ^ b if n & (n - 1) == 0 else (a + b) % n


def uncomb(k, d, n):
    return k ^ d if n & (n - 1) == 0 else (k + d) % n


def gram_kernel(where, *refs, pieces, rows, columns, tile, aliased):
    refs = refs[1:] if aliased else refs
    left, scale = refs[:2]
    parts = refs[2 : 2 + pieces]
    out = refs[2 + pieces]
    right, held, sems = refs[3 + pieces :]
    at = 0
    for part in parts:
        n = part.shape[0]
        right[at : at + n, :] = part[:, :columns]
        at += n
    factor = scale[0:1, 0:1]
    start = pl.multiple_of(where[0] * columns, LANES)
    copies = []
    for i in range(rows // tile):
        held[i] = (
            lax.dot_general(
                left[i * tile : (i + 1) * tile, :], right[...], (((1,), (0,)), ((), ())), preferred_element_type=F32
            )
            * factor
        )
        copies.append(
            pltpu.make_async_copy(
                held.at[i], out.at[0, pl.ds(i * tile, tile), pl.ds(start, columns)], sems.at[i]
            )
        )
        copies[-1].start()
    for copy in copies:
        copy.wait()


def gram(where, left, scale, parts, before, columns, width):
    rows, tokens = left.shape
    tile = next(t for t in (128, 112, 64, 56, 32, 16, 8, rows) if rows % t == 0)
    n = len(parts)
    specs = [pl.BlockSpec(memory_space=pltpu.VMEM)] * (2 + n)
    args = [left, scale, *parts]
    if before is not None:
        specs, args = [pl.BlockSpec(memory_space=pl.ANY)] + specs, [before] + args
    return pl.pallas_call(
        functools.partial(
            gram_kernel, pieces=n, rows=rows, columns=columns, tile=tile, aliased=before is not None
        ),
        grid_spec=pltpu.PrefetchScalarGridSpec(
            num_scalar_prefetch=1,
            grid=(),
            in_specs=specs,
            out_specs=pl.BlockSpec(memory_space=pl.ANY),
            scratch_shapes=[
                pltpu.VMEM((tokens, columns), BF16),
                pltpu.VMEM((rows // tile, tile, columns), F32),
                pltpu.SemaphoreType.DMA((rows // tile,)),
            ],
        ),
        out_shape=jax.ShapeDtypeStruct((1, rows, width), F32),
        input_output_aliases={} if before is None else {1: 0},
        compiler_params=pltpu.CompilerParams(vmem_limit_bytes=30 * 2**20),
        cost_estimate=pl.CostEstimate(
            flops=2 * rows * tokens * columns, bytes_accessed=4 * rows * columns, transcendentals=0
        ),
        name="gram",
    )(where, *args)


def left_kernel(where, *refs, rows, columns):
    parts, (left, scale) = refs[:-2], refs[-2:]
    start = pl.multiple_of(where[0] * rows, LANES)
    chosen = jnp.concatenate([part[:, pl.ds(start, rows)].astype(F32) for part in parts], axis=0)
    left[...] = chosen.T.astype(BF16)
    count = sum(jnp.sum(part[:, columns:].astype(F32), axis=0, keepdims=True) for part in parts)
    scale[...] = jnp.broadcast_to(2.0 / count, scale.shape)


def left_operand(where, parts, rows, columns):
    tokens = sum(part.shape[0] for part in parts)
    if rows % LANES:
        whole = jnp.concatenate(parts, axis=0)
        chosen = lax.dynamic_slice_in_dim(whole, where[0] * rows, rows, 1)
        count = jnp.sum(whole[:, columns].astype(F32))
        return chosen.T, jnp.full((8, LANES), 2.0 / count, F32)
    return pl.pallas_call(
        functools.partial(left_kernel, rows=rows, columns=columns),
        grid_spec=pltpu.PrefetchScalarGridSpec(
            num_scalar_prefetch=1,
            grid=(),
            in_specs=[pl.BlockSpec(memory_space=pltpu.VMEM)] * len(parts),
            out_specs=[pl.BlockSpec(memory_space=pltpu.VMEM)] * 2,
        ),
        out_shape=[jax.ShapeDtypeStruct((rows, tokens), BF16), jax.ShapeDtypeStruct((8, LANES), F32)],
        cost_estimate=pl.CostEstimate(flops=rows * tokens * 64, bytes_accessed=4 * rows * tokens, transcendentals=0),
        name="left",
    )(where, *parts)


def solution(mesh):
    dims = tok_dims(mesh)
    experts = mesh.shape["exp"]
    n0, n1, n2 = dims
    group = n0 * n1 * n2

    def index(c):
        return (c[0] * n1 + c[1]) * n2 + c[2]

    coords = [(a, b, c) for a in range(n0) for b in range(n1) for c in range(n2)]

    def hops(axis_of, d):
        pairs = []
        for c in coords:
            for e in range(experts):
                axis = axis_of(e)
                to = list(c)
                to[axis] = comb(c[axis], d, dims[axis])
                pairs.append((index(c) * experts + e, index(to) * experts + e))
        return pairs

    def send(value, axis_of, d):
        return lax.ppermute(value, ("tok", "exp"), hops(axis_of, d))

    mirrored = n1 == n2
    first = lambda e: 1 + (e + 1) % 2 if mirrored else 2
    second = lambda e: 3 - first(e)

    def shards(activations, expert_ids):
        rows_in, width = activations.shape
        rows = width // group
        chunk = width // n0
        tok, exp = lax.axis_index("tok"), lax.axis_index("exp")
        z = tok // (n1 * n2)
        where = jnp.stack([exp, z]).astype(jnp.int32)
        slots = pl.pallas_call(
            functools.partial(slots_kernel, experts=experts, blocks=n0, chunk=chunk),
            grid_spec=pltpu.PrefetchScalarGridSpec(
                num_scalar_prefetch=1,
                grid=(),
                in_specs=[pl.BlockSpec(memory_space=pltpu.VMEM)] * 2,
                out_specs=pl.BlockSpec(memory_space=pltpu.VMEM),
            ),
            out_shape=jax.ShapeDtypeStruct((experts, CAP, width + LANES), BF16),
            name="slots",
        )(where, expert_ids, activations)
        mine = [slots[0]]
        for j in range(1, experts):
            mine.append(lax.ppermute(slots[j], "exp", [(e, (e + j) % experts) for e in range(experts)]))
        marks = jnp.concatenate([m[:, width:] for m in mine], axis=0)

        def block(b, marked):
            value = jnp.concatenate([m[:, b * chunk : (b + 1) * chunk] for m in mine], axis=0)
            return jnp.concatenate([value, marks], axis=1) if marked else value

        place = (tok % (n1 * n2)).astype(jnp.int32)[None]
        out = left = scale = None
        for k in range(n0):
            line = [block(k, k == 0)]
            for d in range(1, n0):
                line.append(send(block(uncomb(k, d, n0), k == 0), lambda e: 0, d))
            half = jnp.concatenate(line, axis=0)
            plane = [half] + [send(half, first, d) for d in range(1, dims[first(0)])]
            half = jnp.concatenate(plane, axis=0)
            parts = [half] + [send(half, second, d) for d in range(1, dims[second(0)])]
            if k == 0:
                left, scale = left_operand(place, parts, rows, chunk)
            at = comb(z, k, n0).astype(jnp.int32)[None]
            out = gram(at, left, scale, parts, out, chunk, width)
        return out

    in_specs = (P(("tok", "exp"), None), P(("tok", "exp"), None))
    return jax.shard_map(shards, mesh=mesh, in_specs=in_specs, out_specs=P("exp", "tok", None), check_vma=False)
```
